8 devices in a mesh: dp: 2 (over z, y), cp: 4 (over x, core).
Axes of the slice: x: 2, y: 2, z: 1, core: 2. Of those that a mesh axis runs over, the one named last changes fastest.
Arguments:
- x_in: bfloat16 [6, 1536, 2048], P('dp', 'cp'), parts along dimension 0
- positions: int32 [3072], P(('dp', 'cp')), parts along dimension 0
- long_factor: float32 [32], replicated
- norm_gain: float32 [2048], replicated
- w_qkv: bfloat16 [2048, 6144], replicated
- w_out: bfloat16 [2048, 2048], replicated
- grad_y: bfloat16 [6, 1536, 2048], P('dp', 'cp'), parts along dimension 0
Outputs:
- output 1: bfloat16 [6, 1536, 2048], P('dp', 'cp'), parts along dimension 0
- output 2: bfloat16 [6, 1536, 2048], P('dp', 'cp'), parts along dimension 0
- output 3: float32 [4096], P('dp'), parts along dimension 0
- output 4: float32 [4096, 6144], P('dp'), parts along dimension 0
- output 5: float32 [4096, 2048], P('dp'), parts along dimension 0
There are 2 independent parts. The reference program is written for one: setup_inputs(seed, part) draws one part's arguments, and reference() takes and returns one part's arrays. A program takes and returns all parts, laid end to end along the dimension named above; an argument that names none is the same for every part.
All inputs are finite; a program needn't handle non-finite values.
Results may differ from the reference program's by a relative error of at most 0.01427.
Values are sent between devices in bfloat16 or wider.
A program may use at most 1 GiB of HBM per device.

```python
import math
import jax
import jax.numpy as jnp
from jax import lax

BATCH = 3
SEQ_LEN = 1536
HIDDEN = 2048
HEADS = 32
HEAD_DIM = 64
HALF_DIM = HEAD_DIM // 2
WIDTH = HEADS * HEAD_DIM
NORM_EPS = 1e-5
MSCALE = math.sqrt(1.0 + math.log(32.0) / math.log(4096.0))
SCALE = 1.0 / math.sqrt(HEAD_DIM)
QK_GAIN = 1.6
MASK_VALUE = -1e30


def setup_inputs(seed: int = 0, part: int = 0) -> dict:
    part_keys = jax.random.split(jax.random.fold_in(jax.random.key(seed), part), 3)
    shared_keys = jax.random.split(jax.random.key(seed + 1), 4)
    x_in = jax.random.normal(part_keys[0], (BATCH, SEQ_LEN, HIDDEN), jnp.float32)
    gaps = jax.random.randint(part_keys[1], (SEQ_LEN,), 1, 3)
    positions = (jnp.cumsum(gaps) - 1).astype(jnp.int32)
    grad_y = jax.random.normal(part_keys[2], (BATCH, SEQ_LEN, HIDDEN), jnp.float32)
    long_factor = jnp.exp(jax.random.uniform(shared_keys[0], (HALF_DIM,), jnp.float32, 0.0, 2.5))
    norm_gain = jax.random.uniform(shared_keys[1], (HIDDEN,), jnp.float32, 0.5, 1.5)
    col_gain = jnp.concatenate([jnp.full((2 * WIDTH,), QK_GAIN, jnp.float32), jnp.ones((WIDTH,), jnp.float32)])
    w_qkv = jax.random.normal(shared_keys[2], (HIDDEN, 3 * WIDTH), jnp.float32) * (HIDDEN ** -0.5) * col_gain
    w_out = jax.random.normal(shared_keys[3], (WIDTH, HIDDEN), jnp.float32) * (WIDTH ** -0.5)
    return {'x_in': x_in.astype(jnp.bfloat16), 'positions': positions, 'long_factor': long_factor, 'norm_gain': norm_gain, 'w_qkv': w_qkv.astype(jnp.bfloat16), 'w_out': w_out.astype(jnp.bfloat16), 'grad_y': grad_y.astype(jnp.bfloat16)}


def rope_tables(positions, long_factor):
    exponent = jnp.arange(HALF_DIM, dtype=jnp.float32) * (2.0 / HEAD_DIM)
    inv_freq = 1.0 / (long_factor * jnp.power(10000.0, exponent))
    angles = positions.astype(jnp.float32)[:, None] * inv_freq[None, :]
    angle_pair = jnp.concatenate([angles, angles], axis=-1)
    return jnp.cos(angle_pair) * MSCALE, jnp.sin(angle_pair) * MSCALE


def rotate_half(values):
    return jnp.concatenate([-values[..., HALF_DIM:], values[..., :HALF_DIM]], axis=-1)


def head_attention(blocks):
    q_head, k_head, v_head = blocks
    scores = jnp.einsum('bqd,bkd->bqk', q_head.astype(jnp.float32), k_head.astype(jnp.float32)) * SCALE
    token_idx = jnp.arange(SEQ_LEN)
    scores = jnp.where(token_idx[None, :, None] >= token_idx[None, None, :], scores, MASK_VALUE)
    attn_probs = jax.nn.softmax(scores, axis=-1).astype(jnp.bfloat16)
    return jnp.einsum('bqk,bkd->bqd', attn_probs.astype(jnp.float32), v_head.astype(jnp.float32)).astype(jnp.bfloat16)


def heads_first(tensor):
    return jnp.transpose(tensor, (2, 0, 1, 3))


def block_forward(x_in, norm_gain, w_qkv32, w_out32, cos_tab, sin_tab):
    x_float = x_in.astype(jnp.float32)
    inv_rms = lax.rsqrt(jnp.mean(x_float * x_float, axis=-1, keepdims=True) + NORM_EPS)
    normed = (x_float * inv_rms * norm_gain).astype(jnp.bfloat16)
    qkv_all = jnp.dot(normed.reshape(BATCH * SEQ_LEN, HIDDEN).astype(jnp.float32), w_qkv32)
    qkv_all = qkv_all.reshape(BATCH, SEQ_LEN, 3, HEADS, HEAD_DIM)
    cos_b = cos_tab[None, :, None, :]
    sin_b = sin_tab[None, :, None, :]
    q_rot = (qkv_all[:, :, 0] * cos_b + rotate_half(qkv_all[:, :, 0]) * sin_b).astype(jnp.bfloat16)
    k_rot = (qkv_all[:, :, 1] * cos_b + rotate_half(qkv_all[:, :, 1]) * sin_b).astype(jnp.bfloat16)
    v_val = qkv_all[:, :, 2].astype(jnp.bfloat16)
    attn_out = lax.map(jax.checkpoint(head_attention), (heads_first(q_rot), heads_first(k_rot), heads_first(v_val)))
    attn_flat = jnp.transpose(attn_out, (1, 2, 0, 3)).reshape(BATCH * SEQ_LEN, WIDTH)
    proj = jnp.dot(attn_flat.astype(jnp.float32), w_out32).reshape(BATCH, SEQ_LEN, HIDDEN)
    return (x_float + proj).astype(jnp.bfloat16)


def reference(x_in, positions, long_factor, norm_gain, w_qkv, w_out, grad_y):
    cos_tab, sin_tab = rope_tables(positions, long_factor)

    def run(x_val, gain, w_first, w_second):
        return block_forward(x_val, gain, w_first, w_second, cos_tab, sin_tab)

    y_out, pullback = jax.vjp(run, x_in, norm_gain, w_qkv.astype(jnp.float32), w_out.astype(jnp.float32))
    grad_x, grad_gain, grad_wqkv, grad_wout = pullback(grad_y)
    return y_out, grad_x, grad_gain, grad_wqkv, grad_wout
```

```python
import math
import functools
import jax
import jax.numpy as jnp
from jax import lax
from jax.experimental import pallas as pl
from jax.experimental.pallas import tpu as pltpu
from jax.sharding import PartitionSpec as P

NORM_EPS = 1e-5
MSCALE = math.sqrt(1.0 + math.log(32.0) / math.log(4096.0))
MASK_VALUE = -1e30
VMEM_LIMIT = 60 * 1024 * 1024
NT = (((1,), (1,)), ((), ()))
NN = (((1,), (0,)), ((), ()))
TN = (((0,), (0,)), ((), ()))


def dot(a, b, dims):
    return lax.dot_general(a, b, dims, preferred_element_type=jnp.float32)


def params(semantics):
    return pltpu.CompilerParams(dimension_semantics=semantics, vmem_limit_bytes=VMEM_LIMIT)


def cost(flops, nbytes):
    return pl.CostEstimate(flops=int(flops), bytes_accessed=int(nbytes), transcendentals=0)


def proj_kernel(w_ref, xa_ref, xb_ref, da_ref, db_ref, gain_ref, cos_ref, sin_ref, out_ref, r_ref, dy_ref, *, head_dim, row_blocks, scale):
    step = pl.program_id(1)
    piece = xa_ref.shape[1]
    half = head_dim // 2

    @pl.when(step == 0)
    def _():
        for idx, ref in enumerate((xa_ref, xb_ref)):
            x = ref[0].astype(jnp.float32)
            inv = lax.rsqrt(jnp.mean(x * x, axis=-1, keepdims=True) + NORM_EPS)
            r_ref[0, idx * piece:(idx + 1) * piece, :] = (x * inv * gain_ref[...]).astype(jnp.bfloat16)
        dy_ref[0, :piece, :] = da_ref[0]
        dy_ref[0, piece:, :] = db_ref[0]

    @pl.when(step < 2 * row_blocks)
    def _():
        acc = dot(w_ref[...], r_ref[0], NT)
        factor = jnp.where(step < row_blocks, scale, 1.0).astype(jnp.float32)
        cos = cos_ref[0] * factor
        sin = sin_ref[0] * factor
        for head in range(w_ref.shape[0] // head_dim):
            lo = head * head_dim
            first = acc[lo:lo + half]
            second = acc[lo + half:lo + head_dim]
            out_ref[0, lo:lo + half, :] = (first * cos - second * sin).astype(jnp.bfloat16)
            out_ref[0, lo + half:lo + head_dim, :] = (second * cos + first * sin).astype(jnp.bfloat16)

    @pl.when((step >= 2 * row_blocks) & (step < 3 * row_blocks))
    def _():
        out_ref[0] = dot(w_ref[...], r_ref[0], NT).astype(jnp.bfloat16)

    @pl.when(step >= 3 * row_blocks)
    def _():
        out_ref[0] = dot(w_ref[...], dy_ref[0], NT).astype(jnp.bfloat16)


def project(w_cat, x_own, x_other, dy_own, dy_other, gain, cos, sin, head_dim):
    seqs, piece, hidden = x_own.shape
    rows = w_cat.shape[0]
    block = 512
    steps = rows // block
    pair = 2 * piece
    tok_spec = pl.BlockSpec((1, piece, hidden), lambda s, j: (s, 0, 0))
    tab_spec = pl.BlockSpec((1, head_dim // 2, pair), lambda s, j: (0, 0, 0))
    cat_spec = pl.BlockSpec((1, pair, hidden), lambda s, j: (s, 0, 0))
    return pl.pallas_call(
        functools.partial(proj_kernel, head_dim=head_dim, row_blocks=steps // 4, scale=1.0 / math.sqrt(head_dim)),
        grid=(seqs, steps),
        in_specs=[pl.BlockSpec((block, hidden), lambda s, j: (j, 0)), tok_spec, tok_spec, tok_spec, tok_spec,
                  pl.BlockSpec((1, hidden), lambda s, j: (0, 0)), tab_spec, tab_spec],
        out_specs=[pl.BlockSpec((1, block, pair), lambda s, j: (s, j, 0)), cat_spec, cat_spec],
        out_shape=[jax.ShapeDtypeStruct((seqs, rows, pair), jnp.bfloat16), jax.ShapeDtypeStruct((seqs, pair, hidden), jnp.bfloat16),
                   jax.ShapeDtypeStruct((seqs, pair, hidden), jnp.bfloat16)],
        compiler_params=params(('arbitrary', 'arbitrary')),
        cost_estimate=cost(2 * seqs * pair * hidden * rows, 2 * (rows * hidden + 5 * seqs * pair * hidden)),
        name='project',
    )(w_cat, x_own, x_other, dy_own, dy_other, gain, cos, sin)


def attn_kernel(*refs, head_dim, piece, tile):
    loc_refs, rem_refs = refs[0:4], refs[4:8]
    cos_ref, sin_ref, grads_ref, out_ref, feat, tok, s_scr, p_scr, dk_scr, dv_scr, dq_scr, o_scr = refs[8:]
    half = head_dim // 2
    n_tiles = 4 * piece // tile
    me = lax.axis_index('cp')
    mate = me + 1 - 2 * lax.rem(me, 2)
    places = [me, mate, lax.rem(me + 2, 4), lax.rem(mate + 2, 4)]
    spans = [pl.ds(pl.multiple_of(place * piece, 128), piece) for place in places]
    for idx in range(4):
        for rel in range(4):
            source = (loc_refs, rem_refs)[rel // 2][idx]
            lo = (rel % 2) * piece
            feat[idx, :, spans[rel]] = source[0, :, lo:lo + piece]
    for slot, idx in enumerate((1, 2)):
        tok[slot] = jnp.transpose(feat[idx])
    dk_scr[...] = jnp.zeros_like(dk_scr)
    dv_scr[...] = jnp.zeros_like(dv_scr)
    k_pos = lax.broadcasted_iota(jnp.int32, (tile, tile), 0)
    q_pos = lax.broadcasted_iota(jnp.int32, (tile, tile), 1)
    causal = k_pos <= q_pos

    for qi in range(n_tiles):
        qs = slice(qi * tile, (qi + 1) * tile)
        q_t = feat[0, :, qs]
        do_t = feat[3, :, qs]
        row_max = None
        for ki in range(qi + 1):
            ks = slice(ki * tile, (ki + 1) * tile)
            s = dot(tok[0, ks, :], q_t, NN)
            if ki == qi:
                s = jnp.where(causal, s, MASK_VALUE)
            s_scr[ks, :] = s
            cur = jnp.max(s, axis=0, keepdims=True)
            row_max = cur if row_max is None else jnp.maximum(row_max, cur)
        row_sum = jnp.zeros((1, tile), jnp.float32)
        for ki in range(qi + 1):
            ks = slice(ki * tile, (ki + 1) * tile)
            p = jnp.exp(s_scr[ks, :] - row_max)
            s_scr[ks, :] = p
            row_sum = row_sum + jnp.sum(p, axis=0, keepdims=True)
        inv = 1.0 / row_sum
        o_t = jnp.zeros((head_dim, tile), jnp.float32)
        for ki in range(qi + 1):
            ks = slice(ki * tile, (ki + 1) * tile)
            p = s_scr[ks, :] * inv
            s_scr[ks, :] = p
            p_low = p.astype(jnp.bfloat16)
            p_scr[ks, :] = p_low
            o_t = o_t + dot(feat[2, :, ks], p_low, NN)
        o_scr[:, qs] = o_t.astype(jnp.bfloat16)
        delta = jnp.sum(do_t.astype(jnp.float32) * o_t, axis=0, keepdims=True)
        dq_t = jnp.zeros((head_dim, tile), jnp.float32)
        for ki in range(qi + 1):
            ks = slice(ki * tile, (ki + 1) * tile)
            dp = dot(tok[1, ks, :], do_t, NN)
            ds = (s_scr[ks, :] * (dp - delta)).astype(jnp.bfloat16)
            dq_t = dq_t + dot(feat[1, :, ks], ds, NN)
            dk_scr[:, ks] += dot(q_t, ds, NT)
            dv_scr[:, ks] += dot(do_t, p_scr[ks, :], NT)
        dq_scr[:, qs] = dq_t * (1.0 / math.sqrt(head_dim))

    cos, sin = cos_ref[...], sin_ref[...]
    for slot, scr in enumerate((dq_scr, dk_scr)):
        first, second = scr[:half, :], scr[half:, :]
        scr[:half, :] = first * cos + second * sin
        scr[half:, :] = second * cos - first * sin
    for rel in range(4):
        side, lo = rel // 2, (rel % 2) * piece
        for slot, scr in enumerate((dq_scr, dk_scr, dv_scr)):
            grads_ref[side, slot, :, lo:lo + piece] = scr[:, spans[rel]].astype(jnp.bfloat16)
        out_ref[side, :, lo:lo + piece] = o_scr[:, spans[rel]]


def attention(seq, loc, rem, cos, sin, head_dim, tile=256):
    rows, pair = loc.shape[1:]
    part = rows // 4
    heads = part // head_dim
    length = 2 * pair
    half = head_dim // 2

    def head_spec(which, at):
        return pl.BlockSpec((1, head_dim, pair), lambda h: (at, which * heads + h, 0))

    tab_spec = pl.BlockSpec((half, length), lambda h: (0, 0))
    elems = heads * length * length // 2
    return pl.pallas_call(
        functools.partial(attn_kernel, head_dim=head_dim, piece=pair // 2, tile=tile),
        grid=(heads,),
        in_specs=[head_spec(w, seq) for w in range(4)] + [head_spec(w, 0) for w in range(4)] + [tab_spec, tab_spec],
        out_specs=[pl.BlockSpec((2, 3, head_dim, pair), lambda h: (0, 0, h, 0)), pl.BlockSpec((2, head_dim, pair), lambda h: (0, h, 0))],
        out_shape=[jax.ShapeDtypeStruct((2, 3, part, pair), jnp.bfloat16), jax.ShapeDtypeStruct((2, part, pair), jnp.bfloat16)],
        scratch_shapes=[pltpu.VMEM((4, head_dim, length), jnp.bfloat16), pltpu.VMEM((2, length, head_dim), jnp.bfloat16),
                        pltpu.VMEM((length, tile), jnp.float32), pltpu.VMEM((length, tile), jnp.bfloat16),
                        pltpu.VMEM((head_dim, length), jnp.float32), pltpu.VMEM((head_dim, length), jnp.float32),
                        pltpu.VMEM((head_dim, length), jnp.float32), pltpu.VMEM((head_dim, length), jnp.bfloat16)],
        compiler_params=params(('arbitrary',)),
        cost_estimate=cost(elems * 2 * 256 * 6, 2 * 8 * length * part),
        name='attention',
    )(*([loc] * 4), *([rem] * 4), cos, sin)


def grad_qkv_kernel(*refs):
    out_ref = refs[-1]
    acc = None
    for r_ref, g_refs in ((refs[0], refs[4:7]), ) :
        for seq in range(3):
            term = dot(r_ref[seq], g_refs[seq][0, 0], (((0,), (1,)), ((), ())))
            acc = term if acc is None else acc + term
    for seq in range(3):
        acc = acc + dot(refs[1 + seq][0], refs[4 + seq][1, 0], (((0,), (1,)), ((), ())))
    out_ref[...] = acc


def grad_qkv(r_loc, r_rems, grads, which):
    hidden = r_loc.shape[-1]
    pair = r_loc.shape[1]
    part = grads[0].shape[2]
    bm, bn = 512, 512
    return pl.pallas_call(
        grad_qkv_kernel,
        grid=(part // bn, hidden // bm),
        in_specs=[pl.BlockSpec((3, pair, bm), lambda n, m: (0, 0, m))] + [pl.BlockSpec((1, pair, bm), lambda n, m: (0, 0, m))] * 3
        + [pl.BlockSpec((2, 1, bn, pair), lambda n, m: (0, which, n, 0))] * 3,
        out_specs=pl.BlockSpec((bm, bn), lambda n, m: (m, n)),
        out_shape=jax.ShapeDtypeStruct((hidden, part), jnp.float32),
        compiler_params=params(('arbitrary', 'arbitrary')),
        cost_estimate=cost(2 * 6 * pair * hidden * part, 4 * hidden * part + 12 * pair * (hidden + part)),
        name='grad_qkv',
    )(r_loc, *r_rems, *grads)


def grad_out_kernel(*refs):
    out_ref = refs[-1]
    acc = None
    for seq in range(3):
        term = dot(refs[4 + seq][0], refs[0][seq], NN)
        acc = term if acc is None else acc + term
    for seq in range(3):
        acc = acc + dot(refs[4 + seq][1], refs[1 + seq][0], NN)
    out_ref[...] = acc


def grad_out(dy_loc, dy_rems, outs):
    hidden = dy_loc.shape[-1]
    pair = dy_loc.shape[1]
    part = outs[0].shape[1]
    bm, bn = 512, 512
    return pl.pallas_call(
        grad_out_kernel,
        grid=(hidden // bn, part // bm),
        in_specs=[pl.BlockSpec((3, pair, bn), lambda n, m: (0, 0, n))] + [pl.BlockSpec((1, pair, bn), lambda n, m: (0, 0, n))] * 3
        + [pl.BlockSpec((2, bm, pair), lambda n, m: (0, m, 0))] * 3,
        out_specs=pl.BlockSpec((bm, bn), lambda n, m: (m, n)),
        out_shape=jax.ShapeDtypeStruct((part, hidden), jnp.float32),
        compiler_params=params(('arbitrary', 'arbitrary')),
        cost_estimate=cost(2 * 6 * pair * hidden * part, 4 * hidden * part + 12 * pair * (hidden + part)),
        name='grad_out',
    )(dy_loc, *dy_rems, *outs)


def solution(mesh):
    mate_perm = [(i, i ^ 1) for i in range(4)]
    cross_perm = [(i, i ^ 2) for i in range(4)]

    def device_fn(x_in, positions, long_factor, norm_gain, w_qkv, w_out, grad_y):
        seqs, piece, hidden = x_in.shape
        half = long_factor.shape[0]
        head_dim = 2 * half
        width = w_out.shape[0]
        part = width // 2
        me = lax.axis_index('cp')
        core = lax.rem(me, 2)
        mate = me + 1 - 2 * core

        def to_mate(value):
            return lax.ppermute(value, 'cp', mate_perm)

        def to_cross(value):
            return lax.ppermute(value, 'cp', cross_perm)

        x_mate, dy_mate = to_mate(x_in), to_mate(grad_y)
        remote = []
        for seq in range(seqs):
            x_c, dy_c = to_cross(x_in[seq:seq + 1]), to_cross(grad_y[seq:seq + 1])
            remote.append((x_c, to_mate(x_c), dy_c, to_mate(dy_c)))

        exponent = jnp.arange(half, dtype=jnp.float32) * (1.0 / half)
        inv_freq = 1.0 / (long_factor * jnp.power(10000.0, exponent))
        all_pos = lax.all_gather(positions, 'cp', axis=0, tiled=True)
        angles = inv_freq[:, None] * all_pos.astype(jnp.float32)[None, :]
        cos, sin = jnp.cos(angles) * MSCALE, jnp.sin(angles) * MSCALE

        def rel_table(table, first, second):
            return jnp.concatenate([lax.dynamic_slice_in_dim(table, p * piece, piece, 1) for p in (first, second)], axis=1)[None]

        far, far_mate = lax.rem(me + 2, 4), lax.rem(mate + 2, 4)
        cos_loc, sin_loc = rel_table(cos, me, mate), rel_table(sin, me, mate)
        cos_rem, sin_rem = rel_table(cos, far, far_mate), rel_table(sin, far, far_mate)

        w_own = lax.dynamic_index_in_dim(w_qkv.reshape(hidden, 3, 2, part), core, 2, keepdims=False)
        w_cat = jnp.concatenate([jnp.transpose(w_own, (1, 2, 0)).reshape(3 * part, hidden),
                                 lax.dynamic_slice_in_dim(w_out, core * part, part, 0)], axis=0)
        gain = norm_gain[None, :]

        loc, r_loc, dyc_loc = project(w_cat, x_in, x_mate, grad_y, dy_mate, gain, cos_loc, sin_loc, head_dim)
        r_rems, dy_rems, grads, outs = [], [], [], []
        for seq in range(seqs):
            x_c, x_d, dy_c, dy_d = remote[seq]
            rem, r_rem, dyc_rem = project(w_cat, x_c, x_d, dy_c, dy_d, gain, cos_rem, sin_rem, head_dim)
            grad, out = attention(seq, loc, rem, cos, sin, head_dim)
            r_rems.append(r_rem)
            dy_rems.append(dyc_rem)
            grads.append(grad)
            outs.append(out)

        g_own = jnp.stack([g[0, :, :, :piece] for g in grads])
        g_mate = to_mate(jnp.stack([g[0, :, :, piece:] for g in grads]))
        o_own = jnp.stack([o[0, :, :piece] for o in outs])
        o_mate = to_mate(jnp.stack([o[0, :, piece:] for o in outs]))

        wout_own = grad_out(dyc_loc, dy_rems, outs)
        wout_mate = to_mate(wout_own)
        wqkv_own = [grad_qkv(r_loc, r_rems, grads, which) for which in range(3)]
        wqkv_mate = [to_mate(g) for g in wqkv_own]

        def both(own, other, axis):
            return jnp.concatenate([jnp.where(core == 0, own, other), jnp.where(core == 0, other, own)], axis=axis)

        w_out_own = lax.dynamic_slice_in_dim(w_out, core * part, part, 0)
        w_out_mate = lax.dynamic_slice_in_dim(w_out, (1 - core) * part, part, 0)
        w_mate = lax.dynamic_index_in_dim(w_qkv.reshape(hidden, 3, 2, part), 1 - core, 2, keepdims=False)

        x_float = x_in.astype(jnp.float32)
        proj = jnp.einsum('sht,hd->std', o_own, w_out_own, preferred_element_type=jnp.float32)
        proj = proj + jnp.einsum('sht,hd->std', o_mate, w_out_mate, preferred_element_type=jnp.float32)
        y_out = (x_float + proj).astype(jnp.bfloat16)

        inv_rms = lax.rsqrt(jnp.mean(x_float * x_float, axis=-1, keepdims=True) + NORM_EPS)
        x_hat = x_float * inv_rms
        d_normed = jnp.einsum('scht,dch->std', g_own, w_own, preferred_element_type=jnp.float32)
        d_normed = d_normed + jnp.einsum('scht,dch->std', g_mate, w_mate, preferred_element_type=jnp.float32)
        g_gain = lax.psum(jnp.sum(d_normed * x_hat, axis=(0, 1)), 'cp')
        d_hat = d_normed * norm_gain
        dx_norm = inv_rms * (d_hat - x_hat * jnp.mean(d_hat * x_hat, axis=-1, keepdims=True))
        grad_x = (grad_y.astype(jnp.float32) + dx_norm).astype(jnp.bfloat16)

        g_wqkv = jnp.concatenate([both(a, b, 1) for a, b in zip(wqkv_own, wqkv_mate)], axis=1)
        g_wout = both(wout_own, wout_mate, 0)
        return y_out, grad_x, g_gain, g_wqkv, g_wout

    seq_spec = P('dp', 'cp', None)
    return jax.shard_map(device_fn, mesh=mesh, in_specs=(seq_spec, P(('dp', 'cp')), P(None), P(None), P(None, None), P(None, None), seq_spec), out_specs=(seq_spec, seq_spec, P('dp'), P('dp', None), P('dp', None)), check_vma=False)
```
